128 devices in a mesh: row: 8 (over x, core), col: 16 (over y, z).
Axes of the slice: x: 4, y: 4, z: 4, core: 2. Of those that a mesh axis runs over, the one named last changes fastest.
Arguments:
- factor: float32 [8, 8, 2048, 2048], P(None, None, 'row', 'col'), may hold values from -0.046875 to 0.046875
- inverses: float32 [8, 2048, 2048], P(None, 'col', 'row'), may hold values from -1 to 1
- right_side: float32 [128, 8, 2048], P(None, None, 'row'), may hold values from -6 to 6
Outputs:
- forward_solution: float32 [128, 8, 2048], P(None, None, 'col')
- solution: float32 [128, 8, 2048], P(None, None, 'row')
The draws below stay inside these ranges and needn't reach their ends.
All inputs are finite; a program needn't handle non-finite values.
Results may differ from the reference program's by a relative error of at most 0.00012.
Values sent between devices are 32-bit elements; how exact they have to be, the bound alone decides.
No kernel may reach another device: no remote copies, remote signals or barrier semaphores. Data moves between devices by JAX's collectives and lax.ppermute only.
A program may use at most 64 MiB of HBM per device.

```python
import math
import jax
import jax.numpy as jnp
from jax import lax

ORDER = 16384
BLOCK = 2048
SIDES = 128
BLOCKS = 8


def draw_inverses(key, part):
    key_diagonal, key_lower = jax.random.split(jax.random.fold_in(key, 11))
    diagonal_values = jax.random.uniform(key_diagonal, (BLOCKS, BLOCK), jnp.float32, 0.5, 1.0)
    lower_part = jax.random.truncated_normal(key_lower, -4.0, 4.0, (BLOCKS, BLOCK, BLOCK), jnp.float32)
    lower_part = lower_part * (0.4 / math.sqrt(BLOCK))
    row_numbers = lax.broadcasted_iota(jnp.int32, (BLOCK, BLOCK), 0)
    col_numbers = lax.broadcasted_iota(jnp.int32, (BLOCK, BLOCK), 1)
    strict = (row_numbers > col_numbers).astype(jnp.float32)
    unit_diagonal = (row_numbers == col_numbers).astype(jnp.float32)
    return lower_part * strict[None] + diagonal_values[:, :, None] * unit_diagonal[None]


def steps_of(key, shape, pieces, low, top_value):
    def one(axis_at, blocks):
        draws = jax.random.uniform(jax.random.fold_in(jax.random.fold_in(key, 6), axis_at), (blocks,), jnp.float32, low / len(pieces), top_value / len(pieces))
        return jnp.repeat(jnp.exp(draws), shape[axis_at] // blocks).reshape((-1,) + (1,) * (len(shape) - axis_at - 1))

    gain = one(*pieces[0])
    for cut in pieces[1:]:
        gain = gain * one(*cut)
    return gain


def scatter_about(rng, shape, scale, limit, pieces=(), kind=jnp.bfloat16):
    entries = scale * jax.random.normal(rng, shape, jnp.float32)
    if pieces:
        entries = entries * steps_of(rng, shape, pieces, -0.22, 0.18)
    return jnp.clip(entries, -limit, limit).astype(kind)


def setup_inputs(seed: int = 0) -> dict:
    arg_keys = jax.random.split(jax.random.key(seed), 4)
    return {
        "factor": scatter_about(arg_keys[0], (BLOCKS, BLOCKS, BLOCK, BLOCK), ORDER ** -0.5, 0.046875, ((2, 8), (3, 16)), jnp.float32),
        "inverses": draw_inverses(jax.random.fold_in(arg_keys[3], 71), 0),
        "right_side": scatter_about(arg_keys[2], (SIDES, BLOCKS, BLOCK), 1.0, 6.0, ((2, 8),), jnp.float32),
    }


def reference(factor, inverses, right_side):
    highest = lax.Precision.HIGHEST
    forward = []
    for number in range(BLOCKS):
        target = right_side[:, number]
        if number > 0:
            earlier = jnp.stack(forward, 1)
            target = target - jnp.einsum("sjb,jdb->sd", earlier, factor[number, :number], precision=highest)
        forward.append(jnp.dot(target, inverses[number].T, precision=highest))
    backward = [None] * BLOCKS
    for number in range(BLOCKS - 1, -1, -1):
        target = forward[number]
        if number < BLOCKS - 1:
            later = jnp.stack(backward[number + 1:], 1)
            target = target - jnp.einsum("sid,idb->sb", later, factor[number + 1:, number], precision=highest)
        backward[number] = jnp.dot(target, inverses[number], precision=highest)
    return (jnp.stack(forward, 1), jnp.stack(backward, 1))
```

```python
import jax
import jax.numpy as jnp
from jax import lax
from jax.sharding import Mesh, PartitionSpec as P


HIGH = lax.Precision.HIGH


def total_over(x, axis):
    size = lax.axis_size(axis)
    arrived = [
        lax.ppermute(x, axis, [(i, (i + step) % size) for i in range(size)])
        for step in range(1, size)
    ]
    return x + sum(arrived)


def total_of(x, axes):
    for axis in axes:
        x = total_over(x, axis)
    return x


def local(factor, inverses, right_side):
    total_blocks = factor.shape[0]
    forward = []
    for number in range(total_blocks):
        target = right_side[:, number]
        if number > 0:
            earlier = jnp.stack(forward, 1)
            partial_sum = jnp.einsum(
                "sjb,jdb->sd", earlier, factor[number, :number], precision=HIGH
            )
            target = target - total_of(partial_sum, ("z", "y"))
        contribution = jnp.dot(target, inverses[number].T, precision=HIGH)
        forward.append(total_of(contribution, ("core", "x")))
    backward = [None] * total_blocks
    for number in range(total_blocks - 1, -1, -1):
        target = forward[number]
        if number < total_blocks - 1:
            later = jnp.stack(backward[number + 1 :], 1)
            partial_sum = jnp.einsum(
                "sid,idb->sb", later, factor[number + 1 :, number], precision=HIGH
            )
            target = target - total_of(partial_sum, ("core", "x"))
        contribution = jnp.dot(target, inverses[number], precision=HIGH)
        backward[number] = total_of(contribution, ("z", "y"))
    return (jnp.stack(forward, 1), jnp.stack(backward, 1))


def solution(mesh):
    rows, cols = mesh.devices.shape
    chips = Mesh(mesh.devices.reshape(rows // 2, 2, 4, cols // 4), ("x", "core", "y", "z"))
    row, col = ("x", "core"), ("y", "z")
    placed = (P(None, None, row, col), P(None, col, row), P(None, None, row))
    return jax.shard_map(
        local,
        mesh=chips,
        in_specs=placed,
        out_specs=(P(None, None, col), P(None, None, row)),
        check_vma=False,
    )
```

```python
import jax
import jax.numpy as jnp
from jax import lax
from jax.sharding import Mesh, PartitionSpec as P


HIGH = lax.Precision.HIGH


def product(spec, *arrays):
    return jnp.einsum(spec, *arrays, precision=HIGH, preferred_element_type=jnp.float32)


def total_over(x, axis):
    size = lax.axis_size(axis)
    steps = (1, 3, 2) if size == 4 else range(1, size)
    arrived = [
        lax.ppermute(x, axis, [(i, (i + step) % size) for i in range(size)])
        for step in steps
    ]
    return x + sum(arrived)


def total_of(x, axes):
    for axis in axes:
        x = total_over(x, axis)
    return x


def exchanged(x):
    return lax.all_to_all(x, "z", split_axis=0, concat_axis=0, tiled=True)


def after(x, marker):
    return lax.optimization_barrier((x, marker))[0]


ROW, COL = ("core", "x"), ("z", "y")


def local(factor, inverses, right_side):
    plane = lax.axis_index("z")
    planes = lax.axis_size("z")
    blocks, rows, cols = factor.shape[0], *factor.shape[2:]
    half = blocks // 2
    sides = right_side.shape[0]
    share = sides // planes

    lower, diagonal = {}, {}

    def gather(rows_wanted, first_col, with_inverse, marker=None):
        pieces, places = [], []
        for i in rows_wanted:
            if i > first_col:
                pieces.append(factor[i, first_col : min(i, first_col + half)])
                places += [(i, j) for j in range(first_col, min(i, first_col + half))]
            if with_inverse:
                one = inverses[i].reshape(cols, 2, rows // 2)
                pieces.append(jnp.moveaxis(one, 1, 0).reshape(1, rows, cols))
                places.append(i)
        piece = jnp.concatenate(pieces) if len(pieces) > 1 else pieces[0]
        if marker is not None:
            piece = after(piece, marker)
        whole = lax.all_gather(piece, "z", axis=0)
        for place, item in enumerate(places):
            if isinstance(item, tuple):
                lower[item] = whole[:, place]
            else:
                diagonal[item] = whole[:, place].reshape(planes, 2, cols, rows // 2)

    def down(y, i, j):
        return product("zsc,zrc->sr", y, lower[i, j])

    def solve_down(t, k):
        return product("shb,zhab->zsa", t.reshape(share, 2, rows // 2), diagonal[k])

    def up(x, i, k):
        return product("sr,zrc->zsc", x, lower[i, k])

    def solve_up(u, k):
        return product("zsa,zhab->shb", u, diagonal[k]).reshape(share, rows)

    gather(range(2, half), 0, True)
    b = lax.dynamic_index_in_dim(
        right_side.reshape(planes, share, blocks, rows), plane, 0, keepdims=False
    )

    first = total_of(product("sb,ab->sa", right_side[:, 0], inverses[0]), ROW)
    gather(range(half, half + 2), half, True, first)
    target = right_side[:, 1] - total_of(product("sc,rc->sr", first, factor[1, 0]), COL)
    second = total_of(product("sb,ab->sa", target, inverses[1]), ROW)
    start = jnp.stack([first.reshape(planes, share, cols), second.reshape(planes, share, cols)], 1)
    arrived = exchanged(start)
    y = [arrived[:, 0], arrived[:, 1]]

    far = None
    for k in range(2, blocks):
        if k == half:
            late = exchanged(jnp.stack(y[2:half], 1))
            known = jnp.concatenate([start, late], 1)
            far = exchanged(product("zjsc,ijrc->zisr", known, factor[half:, :half])).sum(0)
        low = k // half * half
        partial = sum((down(y[j], k, j) for j in range(low, k)), 0 if far is None else far[k - half])
        t = b[:, k] - total_over(partial, "y")
        y.append(total_of(solve_down(t, k), ROW))
        if k == 2:
            gather(range(half + 2, blocks), half, True, y[2])
        if k == 3:
            gather(range(2), 0, True, y[3])
        if k == half:
            gather(range(half, blocks), 0, False, y[half])

    whole = lax.all_gather(jnp.stack(y), "z", axis=0)
    whole = lax.dynamic_index_in_dim(whole, plane, 2, keepdims=False)

    x = [None] * blocks
    for k in range(blocks - 1, -1, -1):
        u = y[k]
        if k < blocks - 1:
            u = u - total_of(sum(up(x[i], i, k) for i in range(blocks - 1, k, -1)), ROW)
        x[k] = total_over(solve_up(u, k), "y")

    def placed(parts):
        return jnp.moveaxis(parts, 1, 2).reshape(sides, *parts.shape[1:2], *parts.shape[3:])

    early = lax.all_gather(jnp.stack([x[max(k, 2)] for k in range(blocks)]), "z", axis=0)
    last = jnp.stack([x[0], x[1]])
    last = exchanged(jnp.broadcast_to(last, (planes, *last.shape)))
    return placed(whole), placed(jnp.concatenate([last, early[:, 2:]], 1))


def solution(mesh):
    rows, cols = mesh.devices.shape
    chips = Mesh(mesh.devices.reshape(rows // 2, 2, 4, cols // 4), ("x", "core", "y", "z"))
    row, col = ("x", "core"), ("y", "z")
    placed = (P(None, None, row, col), P(None, col, row), P(None, None, row))
    return jax.shard_map(
        local,
        mesh=chips,
        in_specs=placed,
        out_specs=(P(None, None, col), P(None, None, row)),
        check_vma=False,
    )
```

```python
import jax
import jax.numpy as jnp
from jax import lax
from jax.sharding import Mesh, PartitionSpec as P


HIGH = lax.Precision.HIGH


def product(spec, *arrays):
    return jnp.einsum(spec, *arrays, precision=HIGH, preferred_element_type=jnp.float32)


def shifted(x, axis, step):
    size = lax.axis_size(axis)
    return lax.ppermute(x, axis, [(i, (i + step) % size) for i in range(size)])


def total_over(x, axis):
    steps = (1, 3, 2) if lax.axis_size(axis) == 4 else (1,)
    return x + sum(shifted(x, axis, step) for step in steps)


def total_of(x, axes):
    for axis in axes:
        x = total_over(x, axis)
    return x


def exchanged(x):
    return lax.all_to_all(x, "z", split_axis=0, concat_axis=0, tiled=True)


ROW, COL = ("core", "x"), ("z", "y")
FIRST = 2


def local(factor, inverses, right_side):
    plane = lax.axis_index("z")
    planes = lax.axis_size("z")
    blocks, rows, cols = factor.shape[0], *factor.shape[2:]
    sides = right_side.shape[0]
    share = sides // planes

    lower, diagonal = {}, {}

    def gather(wanted, marker):
        pieces, places = [], []
        blocks_now, inverses_now, _ = lax.optimization_barrier((factor, inverses, marker))
        for i, low, high, with_inverse in wanted:
            if high > low:
                pieces.append(blocks_now[i, low:high])
                places += [(i, j) for j in range(low, high)]
            if with_inverse:
                one = inverses_now[i].reshape(cols, 2, rows // 2)
                pieces.append(jnp.moveaxis(one, 1, 0).reshape(1, rows, cols))
                places.append(i)
        whole = lax.all_gather(jnp.concatenate(pieces), "z", axis=0)
        for place, item in enumerate(places):
            one = whole[:, place]
            if isinstance(item, tuple):
                one = jnp.moveaxis(one, 0, 1).reshape(rows, planes * cols)
                lower[item] = lax.optimization_barrier(one)
            else:
                one = one.reshape(planes, 2, cols, rows // 2)
                one = jnp.moveaxis(one, 1, 2).reshape(planes * cols, rows)
                diagonal[item] = lax.optimization_barrier(one)

    def scattered(x):
        part = lambda step: lax.dynamic_slice_in_dim(x, (plane + step) % planes * share, share, 0)
        return part(0) + sum(shifted(part(step), "z", step) for step in (1, 3, 2))

    b = lax.dynamic_slice_in_dim(right_side, plane * share, share, 0)

    start = []
    contribution = product("sb,ab->sa", right_side[:, 0], inverses[0])
    gather([(2, 2, 2, True), (3, 2, 3, True), (4, 2, 4, True)], contribution)
    start.append(total_of(contribution, ROW))
    target = right_side[:, 1] - total_of(product("sc,rc->sr", start[0], factor[1, 0]), COL)
    contribution = product("sb,ab->sa", target, inverses[1])
    gather([(5, 2, 5, True), (6, 2, 6, True)], contribution)
    start.append(total_of(contribution, ROW))
    known = jnp.stack(start, 1)
    near = scattered(product("sjc,jrc->sr", known, factor[2, :FIRST]))
    far = scattered(product("sjc,ijrc->sir", known, factor[3:, :FIRST]))

    y = [None] * blocks
    for k in range(FIRST, blocks):
        partial = near if k == FIRST else far[:, k - 3]
        for j in range(FIRST, k):
            partial = partial + product("sc,rc->sr", y[j], lower[k, j])
        t = b[:, k] - total_over(partial, "y")
        contribution = product("sb,cb->sc", t, diagonal[k])
        if k == 2:
            gather([(7, 2, 7, True)], contribution)
        if k == 4:
            gather([(0, 0, 0, True), (1, 0, 1, True)] + [(i, 0, 2, False) for i in range(2, blocks)], contribution)
        y[k] = total_of(contribution, ROW)

    pieces = jnp.stack(
        [one.reshape(planes, share, cols) for one in start]
        + [jnp.moveaxis(one.reshape(share, planes, cols), 1, 0) for one in y[FIRST:]]
    )
    whole = lax.all_gather(pieces, "z", axis=0)
    whole = lax.dynamic_index_in_dim(whole, plane, 2, keepdims=False)
    for k in range(FIRST):
        y[k] = jnp.moveaxis(whole[:, k], 0, 1).reshape(share, planes * cols)
    later = jnp.moveaxis(whole[:, FIRST:], 2, 1).reshape(sides, blocks - FIRST, cols)
    forward = jnp.concatenate([known, later], 1)

    x = [None] * blocks
    for k in range(blocks - 1, -1, -1):
        u = y[k]
        if k < blocks - 1:
            partial = 0
            for i in range(blocks - 1, k, -1):
                partial = partial + product("sr,rc->sc", x[i], lower[i, k])
            u = u - total_of(partial, ROW)
        x[k] = total_over(product("sc,cb->sb", u, diagonal[k]), "y")

    early = lax.all_gather(jnp.stack([x[max(k, 2)] for k in range(blocks)], 1), "z", axis=0)
    last = jnp.stack([x[0], x[1]], 1)
    last = exchanged(jnp.broadcast_to(last, (planes, *last.shape)))
    solved = jnp.concatenate([last, early[:, :, 2:]], 2).reshape(sides, blocks, rows)
    return forward, solved


def solution(mesh):
    rows, cols = mesh.devices.shape
    chips = Mesh(mesh.devices.reshape(rows // 2, 2, 4, cols // 4), ("x", "core", "y", "z"))
    row, col = ("x", "core"), ("y", "z")
    placed = (P(None, None, row, col), P(None, col, row), P(None, None, row))
    return jax.shard_map(
        local,
        mesh=chips,
        in_specs=placed,
        out_specs=(P(None, None, col), P(None, None, row)),
        check_vma=False,
    )
```

```python
import functools

import jax
import jax.numpy as jnp
from jax import lax
from jax.experimental import pallas as pl
from jax.experimental.pallas import tpu as pltpu
from jax.sharding import Mesh, PartitionSpec as P


HIGH = lax.Precision.HIGH


def product(spec, *arrays):
    return jnp.einsum(spec, *arrays, precision=HIGH, preferred_element_type=jnp.float32)


def shifted(x, axis, step):
    size = lax.axis_size(axis)
    return lax.ppermute(x, axis, [(i, (i + step) % size) for i in range(size)])


def total_over(x, axis):
    steps = (1, 3, 2) if lax.axis_size(axis) == 4 else (1,)
    return x + sum(shifted(x, axis, step) for step in steps)


def total_of(x, axes):
    for axis in axes:
        x = total_over(x, axis)
    return x


def exchanged(x):
    return lax.all_to_all(x, "z", split_axis=0, concat_axis=0, tiled=True)


def fetch_kernel(wanted, planes, *refs):
    sources, outs, sem = refs[: -len(wanted) - 1], refs[-len(wanted) - 1 : -1], refs[-1]
    copies = []
    for (source, place, beside), out in zip(wanted, outs):
        block = sources[source]
        high, wide = block.shape[-2:]
        for z in range(planes):
            part = block.at[(z, *place)]
            if beside:
                target = out.at[:, pl.ds(z * wide, wide)]
            else:
                target = out.at[pl.ds(z * high, high), :]
            copies.append(pltpu.make_async_copy(part, target, sem.at[len(copies)]))
    for copy in copies:
        copy.start()
    for copy in copies:
        copy.wait()


def fetch(sources, wanted):
    planes = sources[0].shape[0]
    shapes = []
    for source, place, beside in wanted:
        high, wide = sources[source].shape[-2:]
        shapes.append((high, planes * wide) if beside else (planes * high, wide))
    size = sum(4 * a * b for a, b in shapes)
    return pl.pallas_call(
        functools.partial(fetch_kernel, wanted, planes),
        out_shape=[jax.ShapeDtypeStruct(shape, jnp.float32) for shape in shapes],
        in_specs=[pl.BlockSpec(memory_space=pl.ANY)] * len(sources),
        out_specs=[pl.BlockSpec(memory_space=pltpu.VMEM)] * len(wanted),
        scratch_shapes=[pltpu.SemaphoreType.DMA((planes * len(wanted),))],
        cost_estimate=pl.CostEstimate(flops=0, bytes_accessed=2 * size, transcendentals=0),
        name="fetch",
    )(*sources)


ROW, COL = ("core", "x"), ("z", "y")
FIRST = 2


def local(factor, inverses, right_side):
    plane = lax.axis_index("z")
    planes = lax.axis_size("z")
    blocks, rows, cols = factor.shape[0], *factor.shape[2:]
    sides = right_side.shape[0]
    share = sides // planes

    lower, diagonal = {}, {}

    def gathered(top, bottom, left, right, marker):
        now, _ = lax.optimization_barrier((factor, marker))
        return lax.all_gather(now[top:bottom, left:right], "z", axis=0)

    def take(diagonals, region, corner, pairs):
        wanted = [(0, (k,), False) for k in diagonals]
        wanted += [(1, (i - corner[0], j - corner[1]), True) for i, j in pairs]
        got = list(fetch([all_inverses, region], wanted))
        for k in diagonals:
            diagonal[k] = got.pop(0)
        for pair in pairs:
            lower[pair] = got.pop(0)

    def scattered(x):
        part = lambda step: lax.dynamic_slice_in_dim(x, (plane + step) % planes * share, share, 0)
        return part(0) + sum(shifted(part(step), "z", step) for step in (1, 3, 2))

    all_inverses = lax.all_gather(inverses, "z", axis=0)
    b = lax.dynamic_slice_in_dim(right_side, plane * share, share, 0)

    start = []
    contribution = product("sb,ab->sa", right_side[:, 0], inverses[0])
    region_a = gathered(3, 5, 2, 4, contribution)
    start.append(total_of(contribution, ROW))
    target = right_side[:, 1] - total_of(product("sc,rc->sr", start[0], factor[1, 0]), COL)
    contribution = product("sb,ab->sa", target, inverses[1])
    region_b = gathered(5, 7, 2, 6, contribution)
    start.append(total_of(contribution, ROW))
    known = jnp.stack(start, 1)
    near = scattered(product("sjc,jrc->sr", known, factor[2, :FIRST]))
    far = scattered(product("sjc,ijrc->sir", known, factor[3:, :FIRST]))

    y = [None] * blocks
    for k in range(FIRST, blocks):
        if k == 2:
            take([2, 3, 4], region_a, (3, 2), [(3, 2), (4, 2), (4, 3)])
        if k == 5:
            take([5, 6], region_b, (5, 2), [(i, j) for i in (5, 6) for j in range(2, i)])
        if k == 7:
            take([7], region_c, (7, 2), [(7, j) for j in range(2, 7)])
        partial = near if k == FIRST else far[:, k - 3]
        for j in range(FIRST, k):
            partial = partial + product("sc,rc->sr", y[j], lower[k, j])
        t = b[:, k] - total_over(partial, "y")
        contribution = product("sb,cb->sc", t, diagonal[k])
        if k == 2:
            region_c = gathered(7, 8, 2, 7, contribution)
        if k == 4:
            region_d = gathered(1, 8, 0, 2, contribution)
        y[k] = total_of(contribution, ROW)

    pieces = jnp.stack(
        [one.reshape(planes, share, cols) for one in start]
        + [jnp.moveaxis(one.reshape(share, planes, cols), 1, 0) for one in y[FIRST:]]
    )
    whole = lax.all_gather(pieces, "z", axis=0)
    whole = lax.dynamic_index_in_dim(whole, plane, 2, keepdims=False)
    for k in range(FIRST):
        y[k] = jnp.moveaxis(whole[:, k], 0, 1).reshape(share, planes * cols)
    later = jnp.moveaxis(whole[:, FIRST:], 2, 1).reshape(sides, blocks - FIRST, cols)
    forward = jnp.concatenate([known, later], 1)

    x = [None] * blocks
    for k in range(blocks - 1, -1, -1):
        if k == 1:
            pairs = [(i, j) for i in range(1, blocks) for j in range(min(i, 2))]
            take([0, 1], region_d, (1, 0), pairs)
        u = y[k]
        if k < blocks - 1:
            partial = 0
            for i in range(blocks - 1, k, -1):
                partial = partial + product("sr,rc->sc", x[i], lower[i, k])
            u = u - total_of(partial, ROW)
        x[k] = total_over(product("sc,cb->sb", u, diagonal[k]), "y")

    early = lax.all_gather(jnp.stack([x[max(k, 2)] for k in range(blocks)], 1), "z", axis=0)
    last = jnp.stack([x[0], x[1]], 1)
    last = exchanged(jnp.broadcast_to(last, (planes, *last.shape)))
    solved = jnp.concatenate([last, early[:, :, 2:]], 2).reshape(sides, blocks, rows)
    return forward, solved


def solution(mesh):
    rows, cols = mesh.devices.shape
    chips = Mesh(mesh.devices.reshape(rows // 2, 2, 4, cols // 4), ("x", "core", "y", "z"))
    row, col = ("x", "core"), ("y", "z")
    placed = (P(None, None, row, col), P(None, col, row), P(None, None, row))
    return jax.shard_map(
        local,
        mesh=chips,
        in_specs=placed,
        out_specs=(P(None, None, col), P(None, None, row)),
        check_vma=False,
    )
```

```python
import functools

import jax
import jax.numpy as jnp
from jax import lax
from jax.experimental import pallas as pl
from jax.experimental.pallas import tpu as pltpu
from jax.sharding import Mesh, PartitionSpec as P


HIGH = lax.Precision.HIGH


def product(spec, *arrays):
    return jnp.einsum(spec, *arrays, precision=HIGH, preferred_element_type=jnp.float32)


def shifted(x, axis, step):
    size = lax.axis_size(axis)
    return lax.ppermute(x, axis, [(i, (i + step) % size) for i in range(size)])


def total_over(x, axis, beside=()):
    steps = (1, 3, 2) if lax.axis_size(axis) == 4 else (1,)
    arrived = [shifted(x, axis, step) for step in steps]
    arrived, beside = lax.optimization_barrier((arrived, beside))
    return x + sum(arrived), beside


def total_of_rows(x, beside=()):
    x, _ = total_over(x, "core")
    return total_over(x, "x", beside)


def exchanged(x):
    return lax.all_to_all(x, "z", split_axis=0, concat_axis=0, tiled=True)


def copies_of(block, out, col, planes, split):
    high, wide = block.shape[-2:]
    for z in range(planes):
        if split:
            for h in range(2):
                part = block.at[z, pl.ds(h * (high // 2), high // 2)]
                yield part, out.at[pl.ds(z * (high // 2), high // 2), pl.ds(h * wide, wide)]
        else:
            yield block.at[z], out.at[:, pl.ds((col * planes + z) * wide, wide)]


def fetch_kernel(wanted, planes, gathered, *refs):
    outs, sem = refs[:-1], refs[-1]
    copies = []
    for places, out in zip(wanted, outs):
        split = not isinstance(places, tuple)
        for col, place in enumerate((places,) if split else places):
            block = gathered.at[:, place]
            for source, target in copies_of(block, out, col, planes, split):
                copies.append(pltpu.make_async_copy(source, target, sem.at[len(copies)]))
    for copy in copies:
        copy.start()
    for copy in copies:
        copy.wait()


def fetch(gathered, wanted):
    planes, _, high, wide = gathered.shape
    shapes, count = [], 0
    for places in wanted:
        if isinstance(places, tuple):
            shapes.append((high, len(places) * planes * wide))
            count += planes * len(places)
        else:
            shapes.append((planes * high // 2, 2 * wide))
            count += 2 * planes
    size = sum(4 * a * b for a, b in shapes)
    return pl.pallas_call(
        functools.partial(fetch_kernel, wanted, planes),
        out_shape=[jax.ShapeDtypeStruct(shape, jnp.float32) for shape in shapes],
        in_specs=[pl.BlockSpec(memory_space=pl.ANY)],
        out_specs=[pl.BlockSpec(memory_space=pltpu.VMEM)] * len(wanted),
        scratch_shapes=[pltpu.SemaphoreType.DMA((count,))],
        cost_estimate=pl.CostEstimate(flops=300 * size, bytes_accessed=2 * size, transcendentals=0),
        name="fetch",
    )(gathered)


COL = ("z", "y")


def local(factor, inverses, right_side):
    plane = lax.axis_index("z")
    planes = lax.axis_size("z")
    blocks, rows, cols = factor.shape[0], *factor.shape[2:]
    sides = right_side.shape[0]
    share = sides // planes
    wide = planes * cols

    def packed(regions, diagonals, marker):
        now, inverses_now, _ = lax.optimization_barrier((factor, inverses, marker))
        pieces = [now[top:bottom, low:high].reshape(-1, rows, cols) for top, bottom, low, high in regions]
        if diagonals:
            low, high = diagonals
            part = inverses_now[low:high].reshape(high - low, cols, 2, rows // 2)
            pieces.append(jnp.moveaxis(part, 2, 1).reshape(high - low, rows, cols))
        return jnp.concatenate(pieces) if len(pieces) > 1 else pieces[0]

    def gather(piece):
        return lax.all_gather(piece, "z", axis=0)

    def scattered(x, beside=()):
        part = lambda step: lax.dynamic_slice_in_dim(x, (plane + step) % planes * share, share, 0)
        arrived = [shifted(part(step), "z", step) for step in (1, 3, 2)]
        arrived, beside = lax.optimization_barrier((arrived, beside))
        return part(0) + sum(arrived), beside

    b = lax.dynamic_slice_in_dim(right_side, plane * share, share, 0)

    contribution = product("sb,ab->sa", right_side[:, 0], inverses[0])
    group_a = gather(packed([(3, 4, 2, 3), (4, 5, 2, 4)], (2, 5), contribution))
    first, _ = total_of_rows(contribution)
    target, piece_b = total_over(
        product("sc,rc->sr", first, factor[1, 0]),
        "z",
        packed([(5, 6, 2, 5), (6, 7, 2, 6)], (5, 8), first),
    )
    group_b = gather(piece_b)
    target, _ = total_over(target, "y")
    target = right_side[:, 1] - target
    second, _ = total_of_rows(product("sb,ab->sa", target, inverses[1]))
    known = jnp.stack([first, second], 1)
    near = product("sjc,jrc->sr", known, factor[2, :2])

    diagonal, close, rest = {}, {}, {}

    def keep(row, got):
        got = list(got)
        if row in (5, 6, 2, 3, 4):
            diagonal[row] = got.pop(0)
        if row == 5:
            diagonal[7] = got.pop(0)
        if row > 2:
            close[row] = got.pop(0)
        if row > 3:
            rest[row] = got.pop(0)

    fetches = {
        2: lambda: fetch(group_a, [3]),
        3: lambda: fetch(group_a, [4, (0,)]),
        4: lambda: fetch(group_a, [5, (2,), (1,)]),
        5: lambda: fetch(group_b, [7, 9, (2,), (0, 1)]),
        6: lambda: fetch(group_b, [8, (6,), (3, 4, 5)]),
        7: lambda: fetch(group_c, [(4,), (0, 1, 2, 3)]),
    }
    near, got = scattered(near, fetches[2]())
    keep(2, got)
    far_parts = product("sjc,ijrc->sir", known, factor[3:, :2])
    far, _ = scattered(far_parts)

    y = [None] * blocks
    extra = near
    for k in range(2, blocks):
        partial = extra
        if k > 2:
            partial = partial + product("sc,rc->sr", y[k - 1], close[k])
        early = k + 1 in (3, 4, 6)
        total, got = total_over(partial, "y", fetches[k + 1]() if early else ())
        if early:
            keep(k + 1, got)
        contribution = product("sb,cb->sc", b[:, k] - total, diagonal[k])
        beside = ()
        if k + 1 < blocks:
            if not early:
                beside = fetches[k + 1]()
                if k + 1 == 7:
                    piece_d = packed([(1, blocks, 0, 2)], (0, 2), total)
                    beside = (list(beside), piece_d)
            elif k + 1 > 3:
                beside = far[:, k - 2] + product(
                    "sc,rc->sr", jnp.concatenate(y[2:k], 1), rest[k + 1]
                )
            else:
                beside = (far[:, 0], packed([(7, 8, 2, 7)], None, total))
        y[k], beside = total_of_rows(contribution, beside)
        if k + 1 < blocks:
            if not early:
                if k + 1 == 7:
                    beside, piece_d = beside
                    group_d = gather(piece_d)
                keep(k + 1, beside)
                extra = far[:, k - 2] + product(
                    "sc,rc->sr", jnp.concatenate(y[2:k], 1), rest[k + 1]
                )
            elif k == 2:
                extra, piece_c = beside
                group_c = gather(piece_c)
            else:
                extra = beside

    pieces = jnp.stack(
        [one.reshape(planes, share, cols) for one in (first, second)]
        + [jnp.moveaxis(one.reshape(share, planes, cols), 1, 0) for one in y[2:]]
    )
    last_rows = lambda row: (2 * (row - 1), 2 * (row - 1) + 1)
    x = [None] * blocks
    sums = {k: 0 for k in range(blocks)}
    lasts = {}

    def add_rest(row):
        out = product("sr,rc->sc", x[row], rest[row])
        return [sums[k] + out[:, n * wide : (n + 1) * wide] for n, k in enumerate(range(2, row - 1))]

    def add_last(row_list):
        out = sum(product("sr,rc->sc", x[row], lasts[row]) for row in row_list)
        return [sums[k] + out[:, k * wide : (k + 1) * wide] for k in range(2)]

    for k in range(blocks - 1, -1, -1):
        u = y[k]
        if k < blocks - 1:
            partial = sums[k]
            if k >= 2:
                partial = partial + product("sr,rc->sc", x[k + 1], close[k + 1])
            elif k == 1:
                ready = product("sr,rc->sc", x[2], lasts[2])
                sums[0] = sums[0] + ready[:, :wide]
                partial = partial + ready[:, wide:]
            else:
                partial = partial + product("sr,rc->sc", x[1], lasts[1])
            beside = {}
            if k + 1 in rest:
                beside["rest"] = add_rest(k + 1)
            if k == 3:
                beside["fetch"] = fetch(group_d, [last_rows(7), last_rows(6)])
            if k == 2:
                beside["fetch"] = fetch(group_d, [last_rows(3), last_rows(2)])
                beside["last"] = add_last([5, 4])
            total, beside = total_of_rows(partial, beside)
            if "rest" in beside:
                for n, one in enumerate(beside["rest"]):
                    sums[n + 2] = one
            if k == 3:
                lasts[7], lasts[6] = beside["fetch"]
            if k == 2:
                lasts[3], lasts[2] = beside["fetch"]
                sums[0], sums[1] = beside["last"]
            u = u - total
        beside = {}
        if k == 3:
            beside["fetch"] = fetch(group_d, [last_rows(5), last_rows(4)])
            beside["last"] = add_last([7, 6])
        if k == 2:
            beside["fetch"] = fetch(group_d, [(0,), 14, 15])
            beside["last"] = add_last([3])
        x[k], beside = total_over(product("sc,cb->sb", u, diagonal[k]), "y", beside)
        if k == blocks - 2:
            whole = gather(lax.optimization_barrier((pieces, x[k]))[0])
            whole = lax.dynamic_index_in_dim(whole, plane, 2, keepdims=False)
            for one in range(2):
                y[one] = jnp.moveaxis(whole[:, one], 0, 1).reshape(share, wide)
            later = jnp.moveaxis(whole[:, 2:], 2, 1).reshape(sides, blocks - 2, cols)
            forward = jnp.concatenate([known, later], 1)
        if k == 3:
            lasts[5], lasts[4] = beside["fetch"]
            sums[0], sums[1] = beside["last"]
        if k == 2:
            lasts[1], diagonal[0], diagonal[1] = beside["fetch"]
            sums[0], sums[1] = beside["last"]

    early = gather(jnp.stack([x[max(k, 2)] for k in range(blocks)], 1))
    last = jnp.stack([x[0], x[1]], 1)
    last = exchanged(jnp.broadcast_to(last, (planes, *last.shape)))
    solved = jnp.concatenate([last, early[:, :, 2:]], 2).reshape(sides, blocks, rows)
    return forward, solved


def solution(mesh):
    rows, cols = mesh.devices.shape
    chips = Mesh(mesh.devices.reshape(rows // 2, 2, 4, cols // 4), ("x", "core", "y", "z"))
    row, col = ("x", "core"), ("y", "z")
    placed = (P(None, None, row, col), P(None, col, row), P(None, None, row))
    return jax.shard_map(
        local,
        mesh=chips,
        in_specs=placed,
        out_specs=(P(None, None, col), P(None, None, row)),
        check_vma=False,
    )
```

```python
import functools

import jax
import jax.numpy as jnp
from jax import lax
from jax.experimental import pallas as pl
from jax.experimental.pallas import tpu as pltpu
from jax.sharding import Mesh, PartitionSpec as P


HIGH = lax.Precision.HIGH


def product(spec, *arrays):
    return jnp.einsum(spec, *arrays, precision=HIGH, preferred_element_type=jnp.float32)


def shifted(x, axis, step):
    size = lax.axis_size(axis)
    return lax.ppermute(x, axis, [(i, (i + step) % size) for i in range(size)])


def total_over(x, axis, beside=()):
    steps = (2, 3, 1) if lax.axis_size(axis) == 4 else (1,)
    arrived = [shifted(x, axis, step) for step in steps]
    arrived, beside = lax.optimization_barrier((arrived, beside))
    return x + sum(arrived), beside


def total_of_rows(x, beside=()):
    x, _ = total_over(x, "core")
    return total_over(x, "x", beside)


def exchanged(x):
    return lax.all_to_all(x, "z", split_axis=0, concat_axis=0, tiled=True)


def copies_of(block, out, col, planes, split):
    high, wide = block.shape[-2:]
    for z in range(planes):
        if split:
            for h in range(2):
                part = block.at[z, pl.ds(h * (high // 2), high // 2)]
                yield part, out.at[pl.ds(z * (high // 2), high // 2), pl.ds(h * wide, wide)]
        else:
            yield block.at[z], out.at[:, pl.ds((col * planes + z) * wide, wide)]


def fetch_kernel(wanted, planes, gathered, *refs):
    outs, sem = refs[:-1], refs[-1]
    copies = []
    for places, out in zip(wanted, outs):
        split = not isinstance(places, tuple)
        for col, place in enumerate((places,) if split else places):
            block = gathered.at[:, place]
            for source, target in copies_of(block, out, col, planes, split):
                copies.append(pltpu.make_async_copy(source, target, sem.at[len(copies)]))
    for copy in copies:
        copy.start()
    for copy in copies:
        copy.wait()


def fetch(gathered, wanted):
    planes, _, high, wide = gathered.shape
    shapes, count = [], 0
    for places in wanted:
        if isinstance(places, tuple):
            shapes.append((high, len(places) * planes * wide))
            count += planes * len(places)
        else:
            shapes.append((planes * high // 2, 2 * wide))
            count += 2 * planes
    size = sum(4 * a * b for a, b in shapes)
    return pl.pallas_call(
        functools.partial(fetch_kernel, wanted, planes),
        out_shape=[jax.ShapeDtypeStruct(shape, jnp.float32) for shape in shapes],
        in_specs=[pl.BlockSpec(memory_space=pl.ANY)],
        out_specs=[pl.BlockSpec(memory_space=pltpu.VMEM)] * len(wanted),
        scratch_shapes=[pltpu.SemaphoreType.DMA((count,))],
        cost_estimate=pl.CostEstimate(flops=300 * size, bytes_accessed=2 * size, transcendentals=0),
        name="fetch",
    )(gathered)


COL = ("z", "y")


def local(factor, inverses, right_side):
    plane = lax.axis_index("z")
    planes = lax.axis_size("z")
    blocks, rows, cols = factor.shape[0], *factor.shape[2:]
    sides = right_side.shape[0]
    share = sides // planes
    wide = planes * cols

    def packed(regions, diagonals, marker):
        now, inverses_now, _ = lax.optimization_barrier((factor, inverses, marker))
        pieces = [now[top:bottom, low:high].reshape(-1, rows, cols) for top, bottom, low, high in regions]
        if diagonals:
            low, high = diagonals
            part = inverses_now[low:high].reshape(high - low, cols, 2, rows // 2)
            pieces.append(jnp.moveaxis(part, 2, 1).reshape(high - low, rows, cols))
        return jnp.concatenate(pieces) if len(pieces) > 1 else pieces[0]

    def gather(piece):
        return lax.all_gather(piece, "z", axis=0)

    def scattered(x, beside=()):
        part = lambda step: lax.dynamic_slice_in_dim(x, (plane + step) % planes * share, share, 0)
        arrived = [shifted(part(step), "z", step) for step in (2, 3, 1)]
        arrived, beside = lax.optimization_barrier((arrived, beside))
        return part(0) + sum(arrived), beside

    b = lax.dynamic_slice_in_dim(right_side, plane * share, share, 0)

    contribution = product("sb,ab->sa", right_side[:, 0], inverses[0])
    group_a = gather(packed([(3, 4, 2, 3), (4, 5, 2, 4)], (2, 5), contribution))
    first, _ = total_of_rows(contribution)
    target, piece_b = total_over(
        product("sc,rc->sr", first, factor[1, 0]),
        "z",
        packed([(5, 6, 2, 5), (6, 7, 2, 6)], (5, 8), first),
    )
    group_b = gather(piece_b)
    target, _ = total_over(target, "y")
    target = right_side[:, 1] - target
    second, _ = total_of_rows(product("sb,ab->sa", target, inverses[1]))
    known = jnp.stack([first, second], 1)
    near = product("sjc,jrc->sr", known, factor[2, :2])

    diagonal, close, rest = {}, {}, {}

    def keep(row, got):
        got = list(got)
        if row in (5, 6, 2, 3, 4):
            diagonal[row] = got.pop(0)
        if row == 5:
            diagonal[7] = got.pop(0)
        if row > 2:
            close[row] = got.pop(0)
        if row > 3:
            rest[row] = got.pop(0)

    fetches = {
        2: lambda: fetch(group_a, [3]),
        3: lambda: fetch(group_a, [4, (0,)]),
        4: lambda: fetch(group_a, [5, (2,), (1,)]),
        5: lambda: fetch(group_b, [7, 9, (2,), (0, 1)]),
        6: lambda: fetch(group_b, [8, (6,), (3, 4, 5)]),
        7: lambda: fetch(group_c, [(4,), (0, 1, 2, 3)]),
    }
    near, got = scattered(near, fetches[2]())
    keep(2, got)
    far_parts = product("sjc,ijrc->sir", known, factor[3:, :2])
    far, _ = scattered(far_parts)

    y = [None] * blocks
    extra = near
    for k in range(2, blocks):
        partial = extra
        if k > 2:
            partial = partial + product("sc,rc->sr", y[k - 1], close[k])
        early = k + 1 in (3, 4, 6)
        total, got = total_over(partial, "y", fetches[k + 1]() if early else ())
        if early:
            keep(k + 1, got)
        contribution = product("sb,cb->sc", b[:, k] - total, diagonal[k])
        beside = ()
        if k + 1 < blocks:
            if not early:
                beside = fetches[k + 1]()
                if k + 1 == 7:
                    piece_d = packed([(1, blocks, 0, 2)], (0, 2), total)
                    beside = (list(beside), piece_d)
            elif k + 1 > 3:
                beside = far[:, k - 2] + product(
                    "sc,rc->sr", jnp.concatenate(y[2:k], 1), rest[k + 1]
                )
            else:
                beside = (far[:, 0], packed([(7, 8, 2, 7)], None, total))
        y[k], beside = total_of_rows(contribution, beside)
        if k + 1 < blocks:
            if not early:
                if k + 1 == 7:
                    beside, piece_d = beside
                    group_d = gather(piece_d)
                keep(k + 1, beside)
                extra = far[:, k - 2] + product(
                    "sc,rc->sr", jnp.concatenate(y[2:k], 1), rest[k + 1]
                )
            elif k == 2:
                extra, piece_c = beside
                group_c = gather(piece_c)
            else:
                extra = beside

    pieces = jnp.stack(
        [one.reshape(planes, share, cols) for one in (first, second)]
        + [jnp.moveaxis(one.reshape(share, planes, cols), 1, 0) for one in y[2:]]
    )
    last_rows = lambda row: (2 * (row - 1), 2 * (row - 1) + 1)
    x = [None] * blocks
    sums = {k: 0 for k in range(blocks)}
    lasts = {}

    def add_rest(row):
        out = product("sr,rc->sc", x[row], rest[row])
        return [sums[k] + out[:, n * wide : (n + 1) * wide] for n, k in enumerate(range(2, row - 1))]

    def add_last(row_list):
        out = sum(product("sr,rc->sc", x[row], lasts[row]) for row in row_list)
        return [sums[k] + out[:, k * wide : (k + 1) * wide] for k in range(2)]

    for k in range(blocks - 1, -1, -1):
        u = y[k]
        if k < blocks - 1:
            partial = sums[k]
            if k >= 2:
                partial = partial + product("sr,rc->sc", x[k + 1], close[k + 1])
            elif k == 1:
                ready = product("sr,rc->sc", x[2], lasts[2])
                sums[0] = sums[0] + ready[:, :wide]
                partial = partial + ready[:, wide:]
            else:
                partial = partial + product("sr,rc->sc", x[1], lasts[1])
            beside = {}
            if k + 1 in rest:
                beside["rest"] = add_rest(k + 1)
            if k == 3:
                beside["fetch"] = fetch(group_d, [last_rows(7), last_rows(6)])
            if k == 2:
                beside["fetch"] = fetch(group_d, [last_rows(3), last_rows(2)])
                beside["last"] = add_last([5, 4])
            total, beside = total_of_rows(partial, beside)
            if "rest" in beside:
                for n, one in enumerate(beside["rest"]):
                    sums[n + 2] = one
            if k == 3:
                lasts[7], lasts[6] = beside["fetch"]
            if k == 2:
                lasts[3], lasts[2] = beside["fetch"]
                sums[0], sums[1] = beside["last"]
            u = u - total
        beside = {}
        if k == 3:
            beside["fetch"] = fetch(group_d, [last_rows(5), last_rows(4)])
            beside["last"] = add_last([7, 6])
        if k == 2:
            beside["fetch"] = fetch(group_d, [(0,), 14, 15])
            beside["last"] = add_last([3])
        x[k], beside = total_over(product("sc,cb->sb", u, diagonal[k]), "y", beside)
        if k == 3:
            whole = gather(lax.optimization_barrier((pieces, lasts[7]))[0])
            whole = lax.dynamic_index_in_dim(whole, plane, 2, keepdims=False)
            for one in range(2):
                y[one] = jnp.moveaxis(whole[:, one], 0, 1).reshape(share, wide)
            later = jnp.moveaxis(whole[:, 2:], 2, 1).reshape(sides, blocks - 2, cols)
            forward = jnp.concatenate([known, later], 1)
        if k == 3:
            lasts[5], lasts[4] = beside["fetch"]
            sums[0], sums[1] = beside["last"]
        if k == 2:
            lasts[1], diagonal[0], diagonal[1] = beside["fetch"]
            sums[0], sums[1] = beside["last"]

    early = gather(jnp.stack([x[max(k, 2)] for k in range(blocks)], 1))
    last = jnp.stack([x[0], x[1]], 1)
    last = exchanged(jnp.broadcast_to(last, (planes, *last.shape)))
    solved = jnp.concatenate([last, early[:, :, 2:]], 2).reshape(sides, blocks, rows)
    return forward, solved


def solution(mesh):
    rows, cols = mesh.devices.shape
    chips = Mesh(mesh.devices.reshape(rows // 2, 2, 4, cols // 4), ("x", "core", "y", "z"))
    row, col = ("x", "core"), ("y", "z")
    placed = (P(None, None, row, col), P(None, col, row), P(None, None, row))
    return jax.shard_map(
        local,
        mesh=chips,
        in_specs=placed,
        out_specs=(P(None, None, col), P(None, None, row)),
        check_vma=False,
    )
```

```python
import functools

import jax
import jax.numpy as jnp
from jax import lax
from jax.experimental import pallas as pl
from jax.experimental.pallas import tpu as pltpu
from jax.sharding import Mesh, PartitionSpec as P


HIGH = lax.Precision.HIGH


def product(spec, *arrays):
    return jnp.einsum(spec, *arrays, precision=HIGH, preferred_element_type=jnp.float32)


def shifted(x, axis, step):
    size = lax.axis_size(axis)
    return lax.ppermute(x, axis, [(i, (i + step) % size) for i in range(size)])


def total_over(x, axis, beside=()):
    steps = (2, 3, 1) if lax.axis_size(axis) == 4 else (1,)
    arrived = [shifted(x, axis, step) for step in steps]
    arrived, beside = lax.optimization_barrier((arrived, beside))
    return x + sum(arrived), beside


def total_of_rows(x, beside=()):
    x, _ = total_over(x, "core")
    return total_over(x, "x", beside)


def exchanged(x):
    return lax.all_to_all(x, "z", split_axis=0, concat_axis=0, tiled=True)


def copies_of(block, out, col, planes, split):
    high, wide = block.shape[-2:]
    for z in range(planes):
        if split:
            for h in range(2):
                part = block.at[z, pl.ds(h * (high // 2), high // 2)]
                yield part, out.at[pl.ds(z * (high // 2), high // 2), pl.ds(h * wide, wide)]
        else:
            yield block.at[z], out.at[:, pl.ds((col * planes + z) * wide, wide)]


def fetch_kernel(wanted, planes, gathered, *refs):
    outs, sem = refs[:-1], refs[-1]
    copies = []
    for places, out in zip(wanted, outs):
        split = not isinstance(places, tuple)
        for col, place in enumerate((places,) if split else places):
            block = gathered.at[:, place]
            for source, target in copies_of(block, out, col, planes, split):
                copies.append(pltpu.make_async_copy(source, target, sem.at[len(copies)]))
    for copy in copies:
        copy.start()
    for copy in copies:
        copy.wait()


def fetch(gathered, wanted):
    planes, _, high, wide = gathered.shape
    shapes, count = [], 0
    for places in wanted:
        if isinstance(places, tuple):
            shapes.append((high, len(places) * planes * wide))
            count += planes * len(places)
        else:
            shapes.append((planes * high // 2, 2 * wide))
            count += 2 * planes
    size = sum(4 * a * b for a, b in shapes)
    return pl.pallas_call(
        functools.partial(fetch_kernel, wanted, planes),
        out_shape=[pltpu.VMEM(shape, jnp.float32) for shape in shapes],
        in_specs=[pl.BlockSpec(memory_space=pl.ANY)],
        out_specs=[pl.BlockSpec(memory_space=pltpu.VMEM)] * len(wanted),
        scratch_shapes=[pltpu.SemaphoreType.DMA((count,))],
        cost_estimate=pl.CostEstimate(flops=300 * size, bytes_accessed=2 * size, transcendentals=0),
        name="fetch",
    )(gathered)


COL = ("z", "y")


def local(factor, inverses, right_side):
    plane = lax.axis_index("z")
    planes = lax.axis_size("z")
    blocks, rows, cols = factor.shape[0], *factor.shape[2:]
    sides = right_side.shape[0]
    share = sides // planes
    wide = planes * cols

    def packed(regions, diagonals, marker):
        now, inverses_now, _ = lax.optimization_barrier((factor, inverses, marker))
        pieces = [now[top:bottom, low:high].reshape(-1, rows, cols) for top, bottom, low, high in regions]
        if diagonals:
            low, high = diagonals
            part = inverses_now[low:high].reshape(high - low, cols, 2, rows // 2)
            pieces.append(jnp.moveaxis(part, 2, 1).reshape(high - low, rows, cols))
        return jnp.concatenate(pieces) if len(pieces) > 1 else pieces[0]

    def gather(piece):
        return lax.all_gather(piece, "z", axis=0)

    def scattered(x, beside=()):
        part = lambda step: lax.dynamic_slice_in_dim(x, (plane + step) % planes * share, share, 0)
        arrived = [shifted(part(step), "z", step) for step in (2, 3, 1)]
        arrived, beside = lax.optimization_barrier((arrived, beside))
        return part(0) + sum(arrived), beside

    b = lax.dynamic_slice_in_dim(right_side, plane * share, share, 0)

    contribution = product("sb,ab->sa", right_side[:, 0], inverses[0])
    group_a = gather(packed([(3, 4, 2, 3), (4, 5, 2, 4)], (2, 5), contribution))
    first, _ = total_of_rows(contribution)
    target, piece_b = total_over(
        product("sc,rc->sr", first, factor[1, 0]),
        "z",
        packed([(5, 6, 2, 5), (6, 7, 2, 6)], (5, 8), first),
    )
    group_b = gather(piece_b)
    target, _ = total_over(target, "y")
    target = right_side[:, 1] - target
    second, _ = total_of_rows(product("sb,ab->sa", target, inverses[1]))
    known = jnp.stack([first, second], 1)
    near = product("sjc,jrc->sr", known, factor[2, :2])

    diagonal, close, rest = {}, {}, {}

    def keep(row, got):
        got = list(got)
        if row in (5, 6, 2, 3, 4):
            diagonal[row] = got.pop(0)
        if row == 5:
            diagonal[7] = got.pop(0)
        if row > 2:
            close[row] = got.pop(0)
        if row > 3:
            rest[row] = got.pop(0)

    fetches = {
        2: lambda: fetch(group_a, [3]),
        3: lambda: fetch(group_a, [4, (0,)]),
        4: lambda: fetch(group_a, [5, (2,), (1,)]),
        5: lambda: fetch(group_b, [7, 9, (2,), (0, 1)]),
        6: lambda: fetch(group_b, [8, (6,), (3, 4, 5)]),
        7: lambda: fetch(group_c, [(4,), (0, 1, 2, 3)]),
    }
    near, got = scattered(near, fetches[2]())
    keep(2, got)
    known_later = lax.optimization_barrier((known, near))[0]
    far_parts = product("sjc,ijrc->sir", known_later, factor[3:, :2])
    far, _ = scattered(far_parts)

    y = [None] * blocks
    extra = near
    for k in range(2, blocks):
        partial = extra
        if k > 2:
            partial = partial + product("sc,rc->sr", y[k - 1], close[k])
        early = k + 1 in (3, 4, 6)
        beside = fetches[k + 1]() if early else ()
        if k == 4:
            beside = packed([(1, blocks, 0, 2)], (0, 2), partial)
        total, got = total_over(partial, "y", beside)
        if early:
            keep(k + 1, got)
        if k == 4:
            piece_d = got
        contribution = product("sb,cb->sc", b[:, k] - total, diagonal[k])
        beside = ()
        if k + 1 < blocks:
            if not early:
                beside = fetches[k + 1]()
            elif k + 1 > 3:
                beside = far[:, k - 2] + product(
                    "sc,rc->sr", jnp.concatenate(y[2:k], 1), rest[k + 1]
                )
            else:
                beside = (far[:, 0], packed([(7, 8, 2, 7)], None, total))
        y[k], beside = total_of_rows(contribution, beside)
        if k + 1 < blocks:
            if not early:
                keep(k + 1, beside)
                extra = far[:, k - 2] + product(
                    "sc,rc->sr", jnp.concatenate(y[2:k], 1), rest[k + 1]
                )
            elif k == 2:
                extra, piece_c = beside
                group_c = gather(piece_c)
            else:
                extra = beside

    group_d = gather(piece_d)

    pieces = jnp.stack(
        [one.reshape(planes, share, cols) for one in (first, second)]
        + [jnp.moveaxis(one.reshape(share, planes, cols), 1, 0) for one in y[2:]]
    )
    last_rows = lambda row: (2 * (row - 1), 2 * (row - 1) + 1)
    x = [None] * blocks
    sums = {k: 0 for k in range(blocks)}
    lasts = {}

    def add_rest(row):
        out = product("sr,rc->sc", x[row], rest[row])
        return [sums[k] + out[:, n * wide : (n + 1) * wide] for n, k in enumerate(range(2, row - 1))]

    def add_last(row_list):
        out = sum(product("sr,rc->sc", x[row], lasts[row]) for row in row_list)
        return [sums[k] + out[:, k * wide : (k + 1) * wide] for k in range(2)]

    for k in range(blocks - 1, -1, -1):
        u = y[k]
        if k < blocks - 1:
            partial = sums[k]
            if k >= 2:
                partial = partial + product("sr,rc->sc", x[k + 1], close[k + 1])
            elif k == 1:
                ready = product("sr,rc->sc", x[2], lasts[2])
                sums[0] = sums[0] + ready[:, :wide]
                partial = partial + ready[:, wide:]
            else:
                partial = partial + product("sr,rc->sc", x[1], lasts[1])
            beside = {}
            if k + 1 in rest:
                beside["rest"] = add_rest(k + 1)
            if k == 3:
                beside["fetch"] = fetch(group_d, [last_rows(7), last_rows(6)])
            if k == 2:
                beside["fetch"] = fetch(lax.optimization_barrier((group_d, x[3]))[0], [last_rows(3), last_rows(2)])
                beside["last"] = add_last([5, 4])
            total, beside = total_of_rows(partial, beside)
            if "rest" in beside:
                for n, one in enumerate(beside["rest"]):
                    sums[n + 2] = one
            if k == 3:
                lasts[7], lasts[6] = beside["fetch"]
            if k == 2:
                lasts[3], lasts[2] = beside["fetch"]
                sums[0], sums[1] = beside["last"]
            u = u - total
        beside = {}
        if k == 3:
            beside["fetch"] = fetch(lax.optimization_barrier((group_d, u))[0], [last_rows(5), last_rows(4)])
            beside["last"] = add_last([7, 6])
        if k == 2:
            beside["fetch"] = fetch(lax.optimization_barrier((group_d, u))[0], [(0,), 14, 15])
            beside["last"] = add_last([3])
        x[k], beside = total_over(product("sc,cb->sb", u, diagonal[k]), "y", beside)
        if k == 3:
            whole = gather(lax.optimization_barrier((pieces, lasts[7]))[0])
            whole = lax.dynamic_index_in_dim(whole, plane, 2, keepdims=False)
            for one in range(2):
                y[one] = jnp.moveaxis(whole[:, one], 0, 1).reshape(share, wide)
            later = jnp.moveaxis(whole[:, 2:], 2, 1).reshape(sides, blocks - 2, cols)
            forward = jnp.concatenate([known, later], 1)
        if k == 3:
            lasts[5], lasts[4] = beside["fetch"]
            sums[0], sums[1] = beside["last"]
        if k == 2:
            lasts[1], diagonal[0], diagonal[1] = beside["fetch"]
            sums[0], sums[1] = beside["last"]

    early = gather(jnp.stack([x[max(k, 2)] for k in range(blocks)], 1))
    last = jnp.stack([x[0], x[1]], 1)
    last = exchanged(jnp.broadcast_to(last, (planes, *last.shape)))
    solved = jnp.concatenate([last, early[:, :, 2:]], 2).reshape(sides, blocks, rows)
    return forward, solved


def solution(mesh):
    rows, cols = mesh.devices.shape
    chips = Mesh(mesh.devices.reshape(rows // 2, 2, 4, cols // 4), ("x", "core", "y", "z"))
    row, col = ("x", "core"), ("y", "z")
    placed = (P(None, None, row, col), P(None, col, row), P(None, None, row))
    return jax.shard_map(
        local,
        mesh=chips,
        in_specs=placed,
        out_specs=(P(None, None, col), P(None, None, row)),
        check_vma=False,
    )
```

```python
import functools

import jax
import jax.numpy as jnp
from jax import lax
from jax.experimental import pallas as pl
from jax.experimental.pallas import tpu as pltpu
from jax.sharding import Mesh, PartitionSpec as P


HIGH = lax.Precision.HIGH


def product(spec, *arrays):
    return jnp.einsum(spec, *arrays, precision=HIGH, preferred_element_type=jnp.float32)


def shifted(x, axis, step):
    size = lax.axis_size(axis)
    return lax.ppermute(x, axis, [(i, (i + step) % size) for i in range(size)])


def total_over(x, axis, beside=()):
    steps = (2, 3, 1) if lax.axis_size(axis) == 4 else (1,)
    arrived = [shifted(x, axis, step) for step in steps]
    arrived, beside = lax.optimization_barrier((arrived, beside))
    return x + sum(arrived), beside


def total_of_rows(x, beside=()):
    x, _ = total_over(x, "core")
    return total_over(x, "x", beside)


def exchanged(x):
    return lax.all_to_all(x, "z", split_axis=0, concat_axis=0, tiled=True)


def copies_of(block, out, col, planes, split):
    high, wide = block.shape[-2:]
    for z in range(planes):
        if split:
            for h in range(2):
                part = block.at[z, pl.ds(h * (high // 2), high // 2)]
                yield part, out.at[pl.ds(z * (high // 2), high // 2), pl.ds(h * wide, wide)]
        else:
            yield block.at[z], out.at[:, pl.ds((col * planes + z) * wide, wide)]


def fetch_kernel(wanted, planes, gathered, *refs):
    outs, sem = refs[:-1], refs[-1]
    copies = []
    for places, out in zip(wanted, outs):
        split = not isinstance(places, tuple)
        for col, place in enumerate((places,) if split else places):
            block = gathered.at[:, place]
            for source, target in copies_of(block, out, col, planes, split):
                copies.append(pltpu.make_async_copy(source, target, sem.at[len(copies)]))
    for copy in copies:
        copy.start()
    for copy in copies:
        copy.wait()


def fetch(gathered, wanted):
    planes, _, high, wide = gathered.shape
    shapes, count = [], 0
    for places in wanted:
        if isinstance(places, tuple):
            shapes.append((high, len(places) * planes * wide))
            count += planes * len(places)
        else:
            shapes.append((planes * high // 2, 2 * wide))
            count += 2 * planes
    size = sum(4 * a * b for a, b in shapes)
    return pl.pallas_call(
        functools.partial(fetch_kernel, wanted, planes),
        out_shape=[pltpu.VMEM(shape, jnp.float32) for shape in shapes],
        in_specs=[pl.BlockSpec(memory_space=pl.ANY)],
        out_specs=[pl.BlockSpec(memory_space=pltpu.VMEM)] * len(wanted),
        scratch_shapes=[pltpu.SemaphoreType.DMA((count,))],
        cost_estimate=pl.CostEstimate(flops=300 * size, bytes_accessed=2 * size, transcendentals=0),
        name="fetch",
    )(gathered)


COL = ("z", "y")


def local(factor, inverses, right_side):
    plane = lax.axis_index("z")
    planes = lax.axis_size("z")
    blocks, rows, cols = factor.shape[0], *factor.shape[2:]
    sides = right_side.shape[0]
    share = sides // planes
    wide = planes * cols

    def packed(regions, diagonals, marker):
        now, inverses_now, _ = lax.optimization_barrier((factor, inverses, marker))
        pieces = [now[top:bottom, low:high].reshape(-1, rows, cols) for top, bottom, low, high in regions]
        if diagonals:
            low, high = diagonals
            part = inverses_now[low:high].reshape(high - low, cols, 2, rows // 2)
            pieces.append(jnp.moveaxis(part, 2, 1).reshape(high - low, rows, cols))
        return jnp.concatenate(pieces) if len(pieces) > 1 else pieces[0]

    def gather(piece):
        return lax.all_gather(piece, "z", axis=0)

    def part_of(x, step):
        return lax.dynamic_slice_in_dim(x, (plane + planes - step) % planes * share, share, 0)

    def from_here(x):
        return jnp.concatenate([part_of(x, step) for step in range(planes)])

    def scattered(parts, beside=()):
        arrived = [shifted(parts[step], "z", planes - step) for step in (2, 1, 3)]
        arrived, beside = lax.optimization_barrier((arrived, beside))
        return parts[0] + sum(arrived), beside

    def collected(x):
        steps = (2, 3, 1)
        arrived = dict(zip(steps, [shifted(x, "z", step) for step in steps]))
        return jnp.concatenate([x] + [arrived[step] for step in range(1, planes)])

    def cut(x):
        return [x[step * share : (step + 1) * share] for step in range(planes)]

    b = lax.dynamic_slice_in_dim(right_side, plane * share, share, 0)

    contribution = product("sb,ab->sa", right_side[:, 0], inverses[0])
    group_a = gather(packed([(3, 4, 2, 3), (4, 5, 2, 4)], (2, 5), contribution))
    first, _ = total_of_rows(contribution)
    target = product("sc,rc->sr", first, factor[1, 0])
    target, piece_b = scattered(
        [part_of(target, step) for step in range(planes)],
        packed([(5, 6, 2, 5), (6, 7, 2, 6)], (5, 8), first),
    )
    group_b = gather(piece_b)
    target, first_here = total_over(target, "y", from_here(first))
    target = collected(b[:, 1] - target)
    second, _ = total_of_rows(product("sb,ab->sa", target, inverses[1]))
    known = jnp.stack([first_here, second], 1)
    near = product("sjc,jrc->sr", known, factor[2, :2])

    diagonal, close, rest = {}, {}, {}

    def keep(row, got):
        got = list(got)
        if row in (5, 6, 2, 3, 4):
            diagonal[row] = got.pop(0)
        if row == 5:
            diagonal[7] = got.pop(0)
        if row > 2:
            close[row] = got.pop(0)
        if row > 3:
            rest[row] = got.pop(0)

    fetches = {
        2: lambda: fetch(group_a, [3]),
        3: lambda: fetch(group_a, [4, (0,)]),
        4: lambda: fetch(group_a, [5, (2,), (1,)]),
        5: lambda: fetch(group_b, [7, 9, (2,), (0, 1)]),
        6: lambda: fetch(group_b, [8, (6,), (3, 4, 5)]),
        7: lambda: fetch(group_c, [(4,), (0, 1, 2, 3)]),
    }
    near, got = scattered(cut(near), fetches[2]())
    keep(2, got)
    known_later = lax.optimization_barrier((known, near))[0]
    far_parts = product("sjc,ijrc->sir", known_later, factor[3:, :2])
    far, _ = scattered(cut(far_parts))

    y = [None] * blocks
    extra = near
    for k in range(2, blocks):
        partial = extra
        if k > 2:
            partial = partial + product("sc,rc->sr", y[k - 1], close[k])
        early = k + 1 in (3, 4, 6)
        beside = fetches[k + 1]() if early else ()
        if k == 4:
            beside = packed([(1, blocks, 0, 2)], (0, 2), partial)
        total, got = total_over(partial, "y", beside)
        if early:
            keep(k + 1, got)
        if k == 4:
            piece_d = got
        contribution = product("sb,cb->sc", b[:, k] - total, diagonal[k])
        beside = ()
        if k + 1 < blocks:
            if not early:
                got = fetches[k + 1]()
                keep(k + 1, got)
                beside = (
                    list(got),
                    far[:, k - 2]
                    + product("sc,rc->sr", jnp.concatenate(y[2:k], 1), rest[k + 1]),
                )
            elif k + 1 > 3:
                beside = far[:, k - 2] + product(
                    "sc,rc->sr", jnp.concatenate(y[2:k], 1), rest[k + 1]
                )
            else:
                beside = (far[:, 0], packed([(7, 8, 2, 7)], None, total))
        y[k], beside = total_of_rows(contribution, beside)
        if k + 1 < blocks:
            if not early:
                got, extra = beside
                keep(k + 1, got)
            elif k == 2:
                extra, piece_c = beside
                group_c = gather(piece_c)
            else:
                extra = beside

    group_d = gather(piece_d)

    second = from_here(second)

    pieces = jnp.stack(
        [one.reshape(planes, share, cols) for one in (first, second)]
        + [jnp.moveaxis(one.reshape(share, planes, cols), 1, 0) for one in y[2:]]
    )
    last_rows = lambda row: (2 * (row - 1), 2 * (row - 1) + 1)
    x = [None] * blocks
    sums = {k: 0 for k in range(blocks)}
    lasts = {}

    def add_rest(row):
        out = product("sr,rc->sc", x[row], rest[row])
        return [sums[k] + out[:, n * wide : (n + 1) * wide] for n, k in enumerate(range(2, row - 1))]

    def add_last(row_list):
        out = sum(product("sr,rc->sc", x[row], lasts[row]) for row in row_list)
        return [sums[k] + out[:, k * wide : (k + 1) * wide] for k in range(2)]

    for k in range(blocks - 1, -1, -1):
        u = y[k]
        if k < blocks - 1:
            partial = sums[k]
            if k >= 2:
                partial = partial + product("sr,rc->sc", x[k + 1], close[k + 1])
            elif k == 1:
                ready = product("sr,rc->sc", x[2], lasts[2])
                sums[0] = sums[0] + ready[:, :wide]
                partial = partial + ready[:, wide:]
            else:
                partial = partial + product("sr,rc->sc", x[1], lasts[1])
            beside = {}
            if k + 1 in rest:
                beside["rest"] = add_rest(k + 1)
            if k == 3:
                beside["fetch"] = fetch(group_d, [last_rows(7), last_rows(6)])
            if k == 2:
                beside["fetch"] = fetch(lax.optimization_barrier((group_d, x[3]))[0], [last_rows(3), last_rows(2)])
                beside["last"] = add_last([5, 4])
            total, beside = total_of_rows(partial, beside)
            if "rest" in beside:
                for n, one in enumerate(beside["rest"]):
                    sums[n + 2] = one
            if k == 3:
                lasts[7], lasts[6] = beside["fetch"]
            if k == 2:
                lasts[3], lasts[2] = beside["fetch"]
                sums[0], sums[1] = beside["last"]
            u = u - total
        beside = {}
        if k == 3:
            beside["fetch"] = fetch(lax.optimization_barrier((group_d, u))[0], [last_rows(5), last_rows(4)])
            beside["last"] = add_last([7, 6])
        if k == 2:
            beside["fetch"] = fetch(lax.optimization_barrier((group_d, u))[0], [(0,), 14, 15])
            beside["last"] = add_last([3])
        x[k], beside = total_over(product("sc,cb->sb", u, diagonal[k]), "y", beside)
        if k == 3:
            whole = gather(lax.optimization_barrier((pieces, lasts[7]))[0])
            whole = lax.dynamic_index_in_dim(whole, plane, 2, keepdims=False)
            for one in range(2):
                y[one] = jnp.moveaxis(whole[:, one], 0, 1).reshape(share, wide)
            later = jnp.moveaxis(whole[:, 2:], 2, 1).reshape(sides, blocks - 2, cols)
            forward = jnp.concatenate([jnp.stack([first, second], 1), later], 1)
        if k == 3:
            lasts[5], lasts[4] = beside["fetch"]
            sums[0], sums[1] = beside["last"]
        if k == 2:
            lasts[1], diagonal[0], diagonal[1] = beside["fetch"]
            sums[0], sums[1] = beside["last"]

    early = gather(jnp.stack([x[max(k, 2)] for k in range(blocks)], 1))
    last = jnp.stack([x[0], x[1]], 1)
    last = exchanged(jnp.broadcast_to(last, (planes, *last.shape)))
    solved = jnp.concatenate([last, early[:, :, 2:]], 2).reshape(sides, blocks, rows)
    return forward, solved


def solution(mesh):
    rows, cols = mesh.devices.shape
    chips = Mesh(mesh.devices.reshape(rows // 2, 2, 4, cols // 4), ("x", "core", "y", "z"))
    row, col = ("x", "core"), ("y", "z")
    placed = (P(None, None, row, col), P(None, col, row), P(None, None, row))
    return jax.shard_map(
        local,
        mesh=chips,
        in_specs=placed,
        out_specs=(P(None, None, col), P(None, None, row)),
        check_vma=False,
    )
```

```python
import functools

import jax
import jax.numpy as jnp
from jax import lax
from jax.experimental import pallas as pl
from jax.experimental.pallas import tpu as pltpu
from jax.sharding import Mesh, PartitionSpec as P


HIGH = lax.Precision.HIGH


def product(spec, *arrays):
    return jnp.einsum(spec, *arrays, precision=HIGH, preferred_element_type=jnp.float32)


def shifted(x, axis, step):
    size = lax.axis_size(axis)
    return lax.ppermute(x, axis, [(i, (i + step) % size) for i in range(size)])


def total_over(x, axis, beside=()):
    steps = (2, 3, 1) if lax.axis_size(axis) == 4 else (1,)
    arrived = [shifted(x, axis, step) for step in steps]
    arrived, beside = lax.optimization_barrier((arrived, beside))
    return x + sum(arrived), beside


def total_of_rows(x, beside=()):
    x, _ = total_over(x, "core")
    return total_over(x, "x", beside)


def exchanged(x):
    return lax.all_to_all(x, "z", split_axis=0, concat_axis=0, tiled=True)


def copies_of(block, out, col, planes, split):
    high, wide = block.shape[-2:]
    for z in range(planes):
        if split:
            for h in range(2):
                part = block.at[z, pl.ds(h * (high // 2), high // 2)]
                yield part, out.at[pl.ds(z * (high // 2), high // 2), pl.ds(h * wide, wide)]
        else:
            yield block.at[z], out.at[:, pl.ds((col * planes + z) * wide, wide)]


def fetch_kernel(wanted, planes, gathered, *refs):
    outs, sem = refs[:-1], refs[-1]
    copies = []
    for places, out in zip(wanted, outs):
        split = not isinstance(places, tuple)
        for col, place in enumerate((places,) if split else places):
            block = gathered.at[:, place]
            for source, target in copies_of(block, out, col, planes, split):
                copies.append(pltpu.make_async_copy(source, target, sem.at[len(copies)]))
    for copy in copies:
        copy.start()
    for copy in copies:
        copy.wait()


def fetch(gathered, wanted):
    planes, _, high, wide = gathered.shape
    shapes, count = [], 0
    for places in wanted:
        if isinstance(places, tuple):
            shapes.append((high, len(places) * planes * wide))
            count += planes * len(places)
        else:
            shapes.append((planes * high // 2, 2 * wide))
            count += 2 * planes
    size = sum(4 * a * b for a, b in shapes)
    return pl.pallas_call(
        functools.partial(fetch_kernel, wanted, planes),
        out_shape=[pltpu.VMEM(shape, jnp.float32) for shape in shapes],
        in_specs=[pl.BlockSpec(memory_space=pl.ANY)],
        out_specs=[pl.BlockSpec(memory_space=pltpu.VMEM)] * len(wanted),
        scratch_shapes=[pltpu.SemaphoreType.DMA((count,))],
        cost_estimate=pl.CostEstimate(flops=300 * size, bytes_accessed=2 * size, transcendentals=0),
        name="fetch",
    )(gathered)


COL = ("z", "y")


def local(factor, inverses, right_side):
    plane = lax.axis_index("z")
    planes = lax.axis_size("z")
    blocks, rows, cols = factor.shape[0], *factor.shape[2:]
    sides = right_side.shape[0]
    share = sides // planes
    wide = planes * cols

    def packed(regions, diagonals, marker):
        now, inverses_now, _ = lax.optimization_barrier((factor, inverses, marker))
        pieces = [now[top:bottom, low:high].reshape(-1, rows, cols) for top, bottom, low, high in regions]
        if diagonals:
            low, high = diagonals
            part = inverses_now[low:high].reshape(high - low, cols, 2, rows // 2)
            pieces.append(jnp.moveaxis(part, 2, 1).reshape(high - low, rows, cols))
        return jnp.concatenate(pieces) if len(pieces) > 1 else pieces[0]

    def gather(piece):
        return lax.all_gather(piece, "z", axis=0)

    def scattered(x, beside=()):
        part = lambda step: lax.dynamic_slice_in_dim(x, (plane + step) % planes * share, share, 0)
        arrived = [shifted(part(step), "z", step) for step in (2, 3, 1)]
        arrived, beside = lax.optimization_barrier((arrived, beside))
        return part(0) + sum(arrived), beside

    b = lax.dynamic_slice_in_dim(right_side, plane * share, share, 0)

    contribution = product("sb,ab->sa", right_side[:, 0], inverses[0])
    group_a = gather(packed([(3, 4, 2, 3), (4, 5, 2, 4)], (2, 5), contribution))
    first, _ = total_of_rows(contribution)
    target, piece_b = total_over(
        product("sc,rc->sr", first, factor[1, 0]),
        "z",
        packed([(5, 6, 2, 5), (6, 7, 2, 6)], (5, 8), first),
    )
    group_b = gather(piece_b)
    target, _ = total_over(target, "y")
    target = right_side[:, 1] - target
    second, _ = total_of_rows(product("sb,ab->sa", target, inverses[1]))
    known = jnp.stack([first, second], 1)
    near = product("sjc,jrc->sr", known, factor[2, :2])

    diagonal, close, rest = {}, {}, {}

    def keep(row, got):
        got = list(got)
        if row in (5, 6, 2, 3, 4):
            diagonal[row] = got.pop(0)
        if row == 5:
            diagonal[7] = got.pop(0)
        if row > 2:
            close[row] = got.pop(0)
        if row > 3:
            rest[row] = got.pop(0)

    fetches = {
        2: lambda: fetch(group_a, [3]),
        3: lambda: fetch(group_a, [4, (0,)]),
        4: lambda: fetch(group_a, [5, (2,), (1,)]),
        5: lambda: fetch(group_b, [7, 9, (2,), (0, 1)]),
        6: lambda: fetch(group_b, [8, (6,), (3, 4, 5)]),
        7: lambda: fetch(group_c, [(4,), (0, 1, 2, 3)]),
    }
    near, got = scattered(near, fetches[2]())
    keep(2, got)
    known_later = lax.optimization_barrier((known, near))[0]
    far_parts = product("sjc,ijrc->sir", known_later, factor[3:, :2])
    far, _ = scattered(far_parts)

    y = [None] * blocks
    extra = near
    for k in range(2, blocks):
        partial = extra
        if k > 2:
            partial = partial + product("sc,rc->sr", y[k - 1], close[k])
        early = k + 1 in (3, 4, 6)
        beside = fetches[k + 1]() if early else ()
        if k == 4:
            beside = packed([(1, blocks, 0, 2)], (0, 2), partial)
        total, got = total_over(partial, "y", beside)
        if early:
            keep(k + 1, got)
        if k == 4:
            piece_d = got
        contribution = product("sb,cb->sc", b[:, k] - total, diagonal[k])
        beside = ()
        if k + 1 < blocks:
            if not early:
                got = fetches[k + 1]()
                keep(k + 1, got)
                beside = (
                    list(got),
                    far[:, k - 2]
                    + product("sc,rc->sr", jnp.concatenate(y[2:k], 1), rest[k + 1]),
                )
            elif k + 1 > 3:
                beside = far[:, k - 2] + product(
                    "sc,rc->sr", jnp.concatenate(y[2:k], 1), rest[k + 1]
                )
            else:
                beside = (far[:, 0], packed([(7, 8, 2, 7)], None, total))
        y[k], beside = total_of_rows(contribution, beside)
        if k + 1 < blocks:
            if not early:
                got, extra = beside
                keep(k + 1, got)
            elif k == 2:
                extra, piece_c = beside
                group_c = gather(piece_c)
            else:
                extra = beside

    group_d = gather(piece_d)

    pieces = jnp.stack(
        [one.reshape(planes, share, cols) for one in (first, second)]
        + [jnp.moveaxis(one.reshape(share, planes, cols), 1, 0) for one in y[2:]]
    )
    last_rows = lambda row: (2 * (row - 1), 2 * (row - 1) + 1)
    x = [None] * blocks
    sums = {k: 0 for k in range(blocks)}
    lasts = {}

    def add_rest(row):
        out = product("sr,rc->sc", x[row], rest[row])
        return [sums[k] + out[:, n * wide : (n + 1) * wide] for n, k in enumerate(range(2, row - 1))]

    def add_last(row_list):
        out = sum(product("sr,rc->sc", x[row], lasts[row]) for row in row_list)
        return [sums[k] + out[:, k * wide : (k + 1) * wide] for k in range(2)]

    for k in range(blocks - 1, -1, -1):
        u = y[k]
        if k < blocks - 1:
            partial = sums[k]
            if k >= 2:
                partial = partial + product("sr,rc->sc", x[k + 1], close[k + 1])
            elif k == 1:
                ready = product("sr,rc->sc", x[2], lasts[2])
                sums[0] = sums[0] + ready[:, :wide]
                partial = partial + ready[:, wide:]
            else:
                partial = partial + product("sr,rc->sc", x[1], lasts[1])
            beside = {}
            if k + 1 in rest:
                beside["rest"] = add_rest(k + 1)
            if k == 3:
                beside["fetch"] = fetch(group_d, [last_rows(7), last_rows(6)])
            if k == 2:
                beside["fetch"] = fetch(lax.optimization_barrier((group_d, x[3]))[0], [last_rows(3), last_rows(2)])
                beside["last"] = add_last([5, 4])
            total, beside = total_of_rows(partial, beside)
            if "rest" in beside:
                for n, one in enumerate(beside["rest"]):
                    sums[n + 2] = one
            if k == 3:
                lasts[7], lasts[6] = beside["fetch"]
            if k == 2:
                lasts[3], lasts[2] = beside["fetch"]
                sums[0], sums[1] = beside["last"]
            u = u - total
        beside = {}
        if k == 3:
            beside["fetch"] = fetch(lax.optimization_barrier((group_d, u))[0], [last_rows(5), last_rows(4)])
            beside["last"] = add_last([7, 6])
        if k == 2:
            beside["fetch"] = fetch(lax.optimization_barrier((group_d, u))[0], [(0,), 14, 15])
            beside["last"] = add_last([3])
        x[k], beside = total_over(product("sc,cb->sb", u, diagonal[k]), "y", beside)
        if k == 3:
            whole = gather(lax.optimization_barrier((pieces, lasts[7]))[0])
            whole = lax.dynamic_index_in_dim(whole, plane, 2, keepdims=False)
            for one in range(2):
                y[one] = jnp.moveaxis(whole[:, one], 0, 1).reshape(share, wide)
            later = jnp.moveaxis(whole[:, 2:], 2, 1).reshape(sides, blocks - 2, cols)
            forward = jnp.concatenate([known, later], 1)
        if k == 3:
            lasts[5], lasts[4] = beside["fetch"]
            sums[0], sums[1] = beside["last"]
        if k == 2:
            lasts[1], diagonal[0], diagonal[1] = beside["fetch"]
            sums[0], sums[1] = beside["last"]

    early = gather(jnp.stack([x[max(k, 2)] for k in range(blocks)], 1))
    last = jnp.stack([x[0], x[1]], 1)
    last = exchanged(jnp.broadcast_to(last, (planes, *last.shape)))
    solved = jnp.concatenate([last, early[:, :, 2:]], 2).reshape(sides, blocks, rows)
    return forward, solved


def solution(mesh):
    rows, cols = mesh.devices.shape
    chips = Mesh(mesh.devices.reshape(rows // 2, 2, 4, cols // 4), ("x", "core", "y", "z"))
    row, col = ("x", "core"), ("y", "z")
    placed = (P(None, None, row, col), P(None, col, row), P(None, None, row))
    return jax.shard_map(
        local,
        mesh=chips,
        in_specs=placed,
        out_specs=(P(None, None, col), P(None, None, row)),
        check_vma=False,
    )
```
